32 devices in a mesh: group: 2 (over y), pages: 4 (over z), heads: 4 (over x, core).
Axes of the slice: x: 2, y: 2, z: 4, core: 2. Of those that a mesh axis runs over, the one named last changes fastest.
Arguments:
- queries: bfloat16 [16, 48, 128], P('group', 'heads'), parts along dimension 0, may hold values from -180 to 180
- k_cache: bfloat16 [8, 16384, 16, 128], P('heads', ('group', 'pages')), parts along dimension 1, may hold values from -6 to 6
- v_cache: bfloat16 [8, 16384, 16, 128], P('heads', ('group', 'pages')), parts along dimension 1, may hold values from -6 to 6
- new_key: bfloat16 [8, 16, 128], P('heads', 'group'), parts along dimension 1, may hold values from -6 to 6
- new_value: bfloat16 [8, 16, 128], P('heads', 'group'), parts along dimension 1, may hold values from -6 to 6
- ctx_lens: int32 [16], P('group'), parts along dimension 0, may hold values from 4081 to 16384, as said below
- page_owner: int32 [16, 1024], P('group'), parts along dimension 0, may hold values from -1 to 3, as said below
- page_slot: int32 [16, 1024], P('group'), parts along dimension 0, may hold values from 0 to 2047, as said below
- out_weight: bfloat16 [6144, 6144], P(None, 'pages'), may hold values from -0.078125 to 0.078125
Outputs:
- projected: bfloat16 [16, 6144], P(('group', 'heads'), 'pages'), parts along dimension 0
The draws below stay inside these ranges and needn't reach their ends.
There are 2 independent parts, one for each index of `group`. The reference program is written for one: setup_inputs(seed, part) draws one part's arguments, and reference() takes and returns one part's arrays. A program takes and returns all parts, laid end to end along the dimension named above; an argument that names none is the same for every part. Nothing has to cross between parts.
Inputs may be any that keep to these rules, and one draw needn't show every extreme that they name: Request r holds ceil(ctx_lens[r] / 16) pages; some request holds 16384 tokens. `page_owner`: for j below request r's page count, the device along pages that holds its logical page j; -1 beyond. No two live pages share a device and a slot. `page_slot`: for j below request r's page count, the slot of logical page j on its device; 0 beyond.
All inputs are finite; a program needn't handle non-finite values.
Results may differ from the reference program's by a relative error of at most 0.0053.
Values may be sent and summed in bfloat16 or wider, within the bound.
A program may use at most 128 MiB of HBM per device.

```python
import math
import jax
import jax.numpy as jnp
from jax import lax

QH = 48
KVH = 8
HD = 128
DM = 6144
PAGE = 16
MAXP = 1024
REQS = 8
PAGES_DEV = 2048
SLOTS_ALL = 8192
N_PAGES = 4


def page_tables(key):
    base_key = jax.random.fold_in(key, 7001)
    count_key, longest_key, tail_key, shuffle_key = jax.random.split(base_key, 4)
    request_ids = jnp.arange(REQS, dtype=jnp.int32)
    fewest = max(MAXP // 4, 1)
    counts = jax.random.randint(count_key, (REQS,), fewest, MAXP + 1, dtype=jnp.int32)
    longest = jax.random.randint(longest_key, (), 0, REQS, dtype=jnp.int32)
    counts = jnp.where(request_ids == longest, MAXP, counts)
    last_rows = jax.random.randint(tail_key, (REQS,), 1, PAGE + 1, dtype=jnp.int32)
    last_rows = jnp.where(request_ids == longest, PAGE, last_rows)
    lengths = (counts - 1) * PAGE + last_rows
    shuffled = jax.random.permutation(shuffle_key, SLOTS_ALL).astype(jnp.int32)
    starts = jnp.cumsum(counts) - counts
    page_number = jnp.arange(MAXP, dtype=jnp.int32)
    flat_index = jnp.clip(starts[:, None] + page_number[None, :], 0, SLOTS_ALL - 1)
    in_use = page_number[None, :] < counts[:, None]
    chosen = shuffled[flat_index]
    page_dev = jnp.where(in_use, chosen // PAGES_DEV, -1).astype(jnp.int32)
    page_local = jnp.where(in_use, chosen % PAGES_DEV, 0).astype(jnp.int32)
    return (lengths.astype(jnp.int32), page_dev, page_local)


def query_base(key):
    drawn = jax.random.normal(jax.random.fold_in(key, 7002), (REQS, QH, HD), jnp.float32)
    return jnp.clip(drawn, -6.0, 6.0)


def draw_queries(key, part):
    base_rows = query_base(key)
    return base_rows.astype(jnp.bfloat16)


def draw_k_cache(key, part):
    drawn = jax.random.normal(jax.random.fold_in(key, 7005), (KVH, SLOTS_ALL, PAGE, HD), jnp.float32)
    drawn_cache = jnp.clip(drawn, -6.0, 6.0)
    return drawn_cache.astype(jnp.bfloat16)


def draw_ctx_lens(key, part):
    return page_tables(key)[0]


def draw_page_owner(key, part):
    return page_tables(key)[1]


def draw_page_slot(key, part):
    return page_tables(key)[2]


def levels(own_key, shape, shards, least, largest):
    level, own = 1.0, jax.random.fold_in(own_key, 6)
    for position, blocks in shards:
        steps = jnp.exp(jax.random.uniform(jax.random.fold_in(own, position), (blocks,), jnp.float32, least / len(shards), largest / len(shards)))
        level = level * jnp.repeat(steps, shape[position] // blocks).reshape([-1 if axis == position else 1 for axis in range(len(shape))])
    return level


def noise(key, shape, spread, most, pieces=(), kind=jnp.bfloat16):
    gain = levels(key, shape, pieces, -0.22, 0.18) if pieces else 1.0
    values = jax.random.normal(key, shape, jnp.float32) * spread * gain
    return jnp.minimum(jnp.maximum(values, -most), most).astype(kind)


def setup_inputs(seed: int = 0, part: int = 0) -> dict:
    arg_keys = jax.random.split(jax.random.key(seed), 10)
    own_keys = jax.random.split(jax.random.fold_in(arg_keys[9], part), 10)
    queries = draw_queries(jax.random.fold_in(jax.random.fold_in(arg_keys[9], part), 71), part)
    k_cache = draw_k_cache(jax.random.fold_in(jax.random.fold_in(arg_keys[9], part), 71), part)
    v_cache = noise(own_keys[2], (KVH, SLOTS_ALL, PAGE, HD), 1.0, 6.0, ((0, 4), (1, 4)))
    new_key = noise(own_keys[3], (KVH, REQS, HD), 1.0, 6.0, ((0, 4),))
    new_value = noise(own_keys[4], (KVH, REQS, HD), 1.0, 6.0, ((0, 4),))
    ctx_lens = draw_ctx_lens(jax.random.fold_in(jax.random.fold_in(arg_keys[9], part), 71), part)
    page_owner = draw_page_owner(jax.random.fold_in(jax.random.fold_in(arg_keys[9], part), 71), part)
    page_slot = draw_page_slot(jax.random.fold_in(jax.random.fold_in(arg_keys[9], part), 71), part)
    out_weight = noise(arg_keys[8], (QH * HD, DM), (QH * HD) ** -0.5, 0.078125, ((1, 4),))
    return {"queries": queries, "k_cache": k_cache, "v_cache": v_cache, "new_key": new_key, "new_value": new_value, "ctx_lens": ctx_lens, "page_owner": page_owner, "page_slot": page_slot, "out_weight": out_weight}


very_low = -1e+30
highest = lax.Precision.HIGHEST

def reference(queries, k_cache, v_cache, new_key, new_value, ctx_lens, page_owner, page_slot, out_weight):
    group_size = QH // KVH
    scaling = 1.0 / math.sqrt(HD)
    row_index = jnp.arange(PAGE, dtype=jnp.int32)
    page_index = jnp.arange(MAXP, dtype=jnp.int32)

    def per_request(operands):
        query, length, page_dev, page_local, key_new, value_new = operands
        global_slot = (jnp.clip(page_dev, 0, N_PAGES - 1) * PAGES_DEV + page_local).astype(jnp.int32)
        gathered_keys = k_cache[:, global_slot].astype(jnp.float32)
        gathered_values = v_cache[:, global_slot].astype(jnp.float32)
        grouped = query.reshape(KVH, group_size, HD).astype(jnp.float32)
        scores = jnp.einsum('kgd,kptd->kgpt', grouped, gathered_keys, precision=highest) * scaling
        live_rows = page_index[:, None] * PAGE + row_index[None, :] < length
        scores = jnp.where(live_rows, scores, very_low)
        page_top = lax.optimization_barrier(jnp.max(scores, axis=3))
        weights = jnp.where(live_rows, jnp.exp(scores - page_top[..., None]), 0.0)
        page_total = lax.optimization_barrier(jnp.sum(weights, axis=3))
        rounded = lax.optimization_barrier(weights.astype(jnp.bfloat16)).astype(jnp.float32)
        page_out = jnp.einsum('kgpt,kptd->kgpd', rounded, gathered_values, precision=highest)
        peak_score = lax.optimization_barrier(jnp.max(page_top, axis=2))
        factor = jnp.exp(page_top - peak_score[..., None])
        partial_out = lax.optimization_barrier(jnp.sum(page_out * factor[..., None], axis=2))
        weight_sum = lax.optimization_barrier(jnp.sum(page_total * factor, axis=2))
        self_score = jnp.einsum('kgd,kd->kg', grouped, key_new.astype(jnp.float32), precision=highest) * scaling
        peak_value = jnp.maximum(peak_score, self_score)
        keep_old = jnp.exp(peak_score - peak_value)
        take_new = jnp.exp(self_score - peak_value)
        attended = (partial_out * keep_old[..., None] + value_new.astype(jnp.float32)[:, None, :] * take_new[..., None]) / (weight_sum * keep_old + take_new)[..., None]
        return attended.reshape(QH * HD).astype(jnp.bfloat16)
    attended = lax.map(per_request, (queries, ctx_lens, page_owner, page_slot, jnp.transpose(new_key, (1, 0, 2)), jnp.transpose(new_value, (1, 0, 2))))
    return jnp.dot(attended, out_weight, preferred_element_type=jnp.float32).astype(jnp.bfloat16)
```

```python
import functools
import math

import jax
import jax.numpy as jnp
from jax import lax
from jax.experimental import pallas as pl
from jax.experimental.pallas import tpu as pltpu
from jax.sharding import PartitionSpec as P

MESH = pl.DeviceIdType.MESH
very_low = -1e30
NT = (((1,), (1,)), ((), ()))


def round_up(value, unit):
    return (value + unit - 1) // unit * unit


def attend_kernel(
    cfg, q_ref, owner_ref, slot_ref, len_ref, k_ref, v_ref, part_ref, buf, s_ref, tok, mx, acc, lsum, ksem, vsem
):
    kv, rows, reqs, blocks, group, page_rows, pages, per_chunk, chunks, factor = cfg
    tokens = per_chunk * page_rows
    depth = q_ref.shape[2]
    own_reqs = reqs // blocks
    kv_block = group * own_reqs
    half = part_ref.shape[1] // 2

    def copy_in(source, sem, c):
        start = pl.multiple_of(c * tokens, tokens)
        return pltpu.make_async_copy(source.at[:, pl.ds(start, tokens)], buf.at[c], sem.at[c])

    for c in range(chunks):
        copy_in(k_ref, ksem, c).start()

    me = lax.axis_index("pages")
    page_id = lax.broadcasted_iota(jnp.int32, (reqs, pages), 1)
    slot = slot_ref[...]
    upper = jnp.where(owner_ref[...] == me, slot // per_chunk, -1)
    lower = slot % per_chunk
    live = jnp.clip(len_ref[...] - page_id * page_rows, 0, page_rows).astype(jnp.float32)
    upper_id = lax.broadcasted_iota(jnp.int32, (chunks, pages), 0)
    lower_id = lax.broadcasted_iota(jnp.int32, (per_chunk, pages), 0)
    table = jnp.zeros((2 * chunks, per_chunk), jnp.float32)
    for r in range(reqs):
        hit = upper[r : r + 1] == upper_id
        left = jnp.concatenate(
            [jnp.where(hit, float(r + 1), 0.0), jnp.where(hit, live[r : r + 1], 0.0)], axis=0
        ).astype(jnp.bfloat16)
        right = jnp.where(lower[r : r + 1] == lower_id, 1.0, 0.0).astype(jnp.bfloat16)
        table += lax.dot_general(left, right, NT, preferred_element_type=jnp.float32)
    spread = jnp.where(
        lax.broadcasted_iota(jnp.int32, (per_chunk, tokens), 1) // page_rows
        == lax.broadcasted_iota(jnp.int32, (per_chunk, tokens), 0),
        1.0,
        0.0,
    ).astype(jnp.bfloat16)
    wide = jnp.dot(table.astype(jnp.bfloat16), spread, preferred_element_type=jnp.float32)
    row_number = (lax.broadcasted_iota(jnp.int32, (chunks, tokens), 1) % page_rows).astype(jnp.float32)
    token_owner = jnp.where(row_number < wide[chunks:], wide[:chunks], 0.0)
    for c in range(chunks):
        tok[c] = jnp.broadcast_to(token_owner[c : c + 1], (8, tokens))

    row_id = lax.broadcasted_iota(jnp.int32, (rows, 128), 0)
    row_req = (row_id // kv_block * own_reqs + row_id % own_reqs + 1).astype(jnp.float32)
    mx[...] = jnp.full_like(mx, very_low)
    acc[...] = jnp.zeros_like(acc)
    lsum[...] = jnp.zeros_like(lsum)
    sub = min(tokens, 512)

    def score_chunk(c, carry):
        copy_in(k_ref, ksem, c).wait()
        for n in range(kv):
            best = [mx[n, 8 * g : 8 * g + 8] for g in range(rows // 8)]
            for b in range(tokens // sub):
                s = lax.dot_general(
                    q_ref[n], buf[c, n, b * sub : (b + 1) * sub, :], NT, preferred_element_type=jnp.float32
                )
                for t in range(sub // 128):
                    at = b * sub + t * 128
                    who = tok[c, :, at : at + 128]
                    for g in range(rows // 8):
                        kept = jnp.where(
                            who == row_req[8 * g : 8 * g + 8],
                            s[8 * g : 8 * g + 8, t * 128 : t * 128 + 128],
                            very_low,
                        )
                        s_ref[c, n, 8 * g : 8 * g + 8, at : at + 128] = kept
                        best[g] = jnp.maximum(best[g], kept)
            for g in range(rows // 8):
                mx[n, 8 * g : 8 * g + 8] = best[g]
        copy_in(v_ref, vsem, c).start()
        return carry

    lax.fori_loop(0, chunks, score_chunk, 0)
    top = jnp.max(mx[...], axis=2, keepdims=True)
    mx[...] = jnp.broadcast_to(top, mx.shape)

    def value_chunk(c, carry):
        copy_in(v_ref, vsem, c).wait()
        for n in range(kv):
            peak = mx[n]
            total = lsum[n]
            out = acc[n]
            for b in range(tokens // sub):
                parts = []
                for t in range(sub // 128):
                    at = b * sub + t * 128
                    w = jnp.exp2((s_ref[c, n, :, at : at + 128] - peak) * factor)
                    total += w
                    parts.append(w.astype(jnp.bfloat16))
                out += jnp.dot(
                    jnp.concatenate(parts, axis=1),
                    buf[c, n, b * sub : (b + 1) * sub, :],
                    preferred_element_type=jnp.float32,
                )
            lsum[n] = total
            acc[n] = out
        return carry

    lax.fori_loop(0, chunks, value_chunk, 0)
    lane = lax.broadcasted_iota(jnp.int32, (rows, 128), 1)
    part_ref[...] = jnp.zeros_like(part_ref)
    for n in range(kv):
        stats = jnp.where(lane == 0, mx[n], jnp.sum(lsum[n], axis=1, keepdims=True))
        out = acc[n]
        for p in range(blocks):
            here = slice(p * kv_block, (p + 1) * kv_block)
            part_ref[p, n * kv_block : (n + 1) * kv_block, :] = out[here]
            part_ref[p, half + n * kv_block : half + (n + 1) * kv_block, :] = stats[here]


def project_kernel(
    cfg, part_ref, q_ref, key_ref, value_ref, w_ref, y_ref,
    wbuf, got, mine, rows_in, lhs, total, wsem, send_a, recv_a, send_b, recv_b,
):
    pages, heads, reqs, head_count, pieces, factor = cfg
    group = lax.axis_index("group")
    p = lax.axis_index("pages")
    h = lax.axis_index("heads")
    half = part_ref.shape[1] // 2
    own_reqs = reqs // pages
    out_reqs = reqs // heads
    shares = pages // heads
    depth = part_ref.shape[2]
    piece_rows = wbuf.shape[1]

    def weight_copy(i):
        return pltpu.make_async_copy(
            w_ref.at[pl.ds(pl.multiple_of(i * piece_rows, piece_rows), piece_rows)], wbuf.at[i], wsem.at[i]
        )

    for i in range(pieces):
        weight_copy(i).start()

    barrier = pltpu.get_barrier_semaphore()
    count = pages * heads
    for k in range(1, count):
        other = lax.rem(p * heads + h + k, count)
        pl.semaphore_signal(
            barrier, inc=1, device_id=(group, other // heads, lax.rem(other, heads)), device_id_type=MESH
        )

    q = q_ref[p]
    self_score = jnp.sum(q * key_ref[p], axis=1, keepdims=True)
    pl.semaphore_wait(barrier, count - 1)

    def exchange(k):
        to = lax.rem(p + k, pages)
        return pltpu.make_async_remote_copy(
            src_ref=part_ref.at[to],
            dst_ref=got.at[k - 1],
            send_sem=send_a.at[k - 1],
            recv_sem=recv_a.at[k - 1],
            device_id=(group, to, h),
            device_id_type=MESH,
        )

    for k in range(1, pages):
        exchange(k).start()
    for k in range(1, pages):
        exchange(k).wait_recv()

    tops = [part_ref[p, half:, 0:1]] + [got[k, half:, 0:1] for k in range(pages - 1)]
    sums = [part_ref[p, half:, 1:2]] + [got[k, half:, 1:2] for k in range(pages - 1)]
    outs = [part_ref[p, :half]] + [got[k, :half] for k in range(pages - 1)]
    peak = self_score
    for t in tops:
        peak = jnp.maximum(peak, t)
    take = jnp.exp2((self_score - peak) * factor)
    out = take * value_ref[p]
    weight = take
    for t, s, o in zip(tops, sums, outs):
        f = jnp.exp2((t - peak) * factor)
        out += f * o
        weight += f * s
    attended = (out / weight).astype(jnp.bfloat16)
    mine[...] = jnp.zeros_like(mine)
    mine[0:half, :] = attended

    target = p // shares
    place = lax.rem(p, shares) * heads + h

    def hand_over(k):
        to = lax.rem(p + k, pages)
        return pltpu.make_async_remote_copy(
            src_ref=mine,
            dst_ref=rows_in.at[place],
            send_sem=send_b.at[k],
            recv_sem=recv_b.at[place],
            device_id=(group, to, target),
            device_id_type=MESH,
        )

    for k in range(pages):
        if k == 0:
            pl.when(target != h)(lambda: hand_over(0).start())

            @pl.when(target == h)
            def _():
                rows_in[place] = mine[...]
        else:
            hand_over(k).start()

    def arrival(source):
        return pltpu.make_async_remote_copy(
            src_ref=mine,
            dst_ref=rows_in.at[source],
            send_sem=send_b.at[0],
            recv_sem=recv_b.at[source],
            device_id=(group, p, target),
            device_id_type=MESH,
        )

    for source in range(shares * heads):
        remote = jnp.logical_or(target != h, place != source)
        pl.when(remote)(lambda source=source: arrival(source).wait_recv())

    lhs[...] = jnp.zeros_like(lhs)
    per_piece = piece_rows // depth
    for source in range(shares * heads):
        first = source // heads * own_reqs
        block = rows_in[source].astype(jnp.float32)
        for n in range(head_count):
            which = source % heads * head_count + n
            col = which % per_piece * depth
            lhs[which // per_piece, first : first + own_reqs, col : col + depth] = block[
                n * own_reqs : (n + 1) * own_reqs
            ]
    total[...] = jnp.zeros_like(total)

    def multiply(i, carry):
        weight_copy(i).wait()
        total[...] += jnp.dot(
            lhs[i].astype(jnp.bfloat16), wbuf[i], preferred_element_type=jnp.float32
        )
        return carry

    lax.fori_loop(0, pieces, multiply, 0)
    y_ref[...] = total[0:out_reqs].astype(jnp.bfloat16)
    for k in range(1, pages):
        exchange(k).wait_send()
    pl.when(target != h)(lambda: hand_over(0).wait_send())
    for k in range(1, pages):
        hand_over(k).wait_send()


def local(sizes, queries, k_cache, v_cache, new_key, new_value, ctx_lens, page_owner, page_slot, out_weight):
    pages, heads = sizes
    kv, slots, page_rows, depth = k_cache.shape
    reqs, q_local, _ = queries.shape
    group = q_local // kv
    max_pages = page_owner.shape[1]
    factor = math.log2(math.e) / math.sqrt(depth)
    per_chunk = math.gcd(slots, 128)
    chunks = slots // per_chunk
    tokens = per_chunk * page_rows
    rows = group * reqs
    own_reqs = reqs // pages
    block = kv * group * own_reqs
    half = round_up(block, 8)
    vmem = pl.BlockSpec(memory_space=pltpu.VMEM)
    hbm = pl.BlockSpec(memory_space=pl.ANY)

    split = queries.reshape(pages, own_reqs, kv, group, depth)
    q_rows = split.transpose(2, 0, 3, 1, 4).reshape(kv, rows, depth)
    cfg = (kv, rows, reqs, pages, group, page_rows, max_pages, per_chunk, chunks, factor)
    part = pl.pallas_call(
        functools.partial(attend_kernel, cfg),
        out_shape=jax.ShapeDtypeStruct((pages, 2 * half, depth), jnp.float32),
        in_specs=[vmem] * 4 + [hbm] * 2,
        out_specs=vmem,
        scratch_shapes=[
            pltpu.VMEM((chunks, kv, tokens, depth), jnp.bfloat16),
            pltpu.VMEM((chunks, kv, rows, tokens), jnp.float32),
            pltpu.VMEM((chunks, 8, tokens), jnp.float32),
            pltpu.VMEM((kv, rows, 128), jnp.float32),
            pltpu.VMEM((kv, rows, depth), jnp.float32),
            pltpu.VMEM((kv, rows, 128), jnp.float32),
            pltpu.SemaphoreType.DMA((chunks,)),
            pltpu.SemaphoreType.DMA((chunks,)),
        ],
        compiler_params=pltpu.CompilerParams(vmem_limit_bytes=48 * 1024 * 1024),
        name="attend",
    )(
        q_rows,
        page_owner,
        page_slot,
        ctx_lens.reshape(reqs, 1),
        k_cache.reshape(kv, slots * page_rows, depth),
        v_cache.reshape(kv, slots * page_rows, depth),
    )

    def padded(x):
        return jnp.pad(x.astype(jnp.float32), ((0, 0), (0, half - block), (0, 0)))

    q_block = padded(split.transpose(0, 2, 3, 1, 4).reshape(pages, block, depth))

    def spread(x):
        y = x.reshape(kv, pages, 1, own_reqs, depth).transpose(1, 0, 2, 3, 4)
        return padded(jnp.broadcast_to(y, (pages, kv, group, own_reqs, depth)).reshape(pages, block, depth))

    model, columns = out_weight.shape
    pieces = math.gcd(model // depth, 8)
    shares = pages // heads
    out_reqs = reqs // heads
    lines = round_up(half, 16)
    cfg = (pages, heads, reqs, q_local, pieces, factor)
    return pl.pallas_call(
        functools.partial(project_kernel, cfg),
        out_shape=jax.ShapeDtypeStruct((out_reqs, columns), jnp.bfloat16),
        in_specs=[vmem] * 4 + [hbm],
        out_specs=vmem,
        scratch_shapes=[
            pltpu.VMEM((pieces, model // pieces, columns), jnp.bfloat16),
            pltpu.VMEM((pages - 1, 2 * half, depth), jnp.float32),
            pltpu.VMEM((lines, depth), jnp.bfloat16),
            pltpu.VMEM((shares * heads, lines, depth), jnp.bfloat16),
            pltpu.VMEM((pieces, 8, model // pieces), jnp.float32),
            pltpu.VMEM((8, columns), jnp.float32),
            pltpu.SemaphoreType.DMA((pieces,)),
            pltpu.SemaphoreType.DMA((pages - 1,)),
            pltpu.SemaphoreType.DMA((pages - 1,)),
            pltpu.SemaphoreType.DMA((pages,)),
            pltpu.SemaphoreType.DMA((shares * heads,)),
        ],
        compiler_params=pltpu.CompilerParams(
            collective_id=0, has_side_effects=True, vmem_limit_bytes=40 * 1024 * 1024
        ),
        name="project",
    )(part, q_block, spread(new_key), spread(new_value), out_weight)


def solution(mesh):
    placed = (
        P("group", "heads", None),
        P("heads", ("group", "pages"), None, None),
        P("heads", ("group", "pages"), None, None),
        P("heads", "group", None),
        P("heads", "group", None),
        P("group"),
        P("group", None),
        P("group", None),
        P(None, "pages"),
    )
    sizes = (mesh.shape["pages"], mesh.shape["heads"])
    return jax.shard_map(
        functools.partial(local, sizes),
        mesh=mesh,
        in_specs=placed,
        out_specs=P(("group", "heads"), "pages"),
        check_vma=False,
    )
```

```python
import functools
import math

import jax
import jax.numpy as jnp
from jax import lax
from jax.experimental import pallas as pl
from jax.experimental.pallas import tpu as pltpu
from jax.sharding import PartitionSpec as P

MESH = pl.DeviceIdType.MESH
very_low = -1e30
NT = (((1,), (1,)), ((), ()))


def round_up(value, unit):
    return (value + unit - 1) // unit * unit


def whole_kernel(
    cfg, q_in, owner_in, slot_in, len_in, key_in, value_in, k_ref, v_ref, w_ref, y_ref,
    q_ref, owner_ref, slot_ref, len_ref, key_ref, value_ref, small_sem, wide_q,
    buf, s_ref, tok, mx, acc, lsum, bsem,
    wbuf, part_ref, got, mine, rows_in, lhs, total, wsem, send_a, recv_a, send_b, recv_b,
):
    pages, heads, page_rows, group, ahead, factor = cfg
    reqs, max_pages = owner_ref.shape
    buffers, kv, tokens, depth = buf.shape
    chunks = s_ref.shape[0]
    rows = group * reqs
    per_chunk = tokens // page_rows
    pieces, piece_rows = wbuf.shape[0], wbuf.shape[1]
    own_reqs = reqs // pages
    out_reqs = reqs // heads
    shares = pages // heads
    half = part_ref.shape[1] // 2
    head_count = kv * group
    replica = lax.axis_index("group")
    p = lax.axis_index("pages")
    h = lax.axis_index("heads")

    def stream(source, c, i):
        at = lax.rem(i, buffers)
        start = pl.multiple_of(c * tokens, tokens)
        return pltpu.make_async_copy(source.at[:, pl.ds(start, tokens)], buf.at[at], bsem.at[at])

    def weight_copy(i):
        return pltpu.make_async_copy(
            w_ref.at[pl.ds(pl.multiple_of(i * piece_rows, piece_rows), piece_rows)], wbuf.at[i], wsem.at[i]
        )

    small = [
        pltpu.make_async_copy(source, target, small_sem.at[i])
        for i, (source, target) in enumerate(
            (
                (owner_in, owner_ref),
                (slot_in, slot_ref),
                (len_in, len_ref),
                (q_in, q_ref),
                (key_in, key_ref),
                (value_in, value_ref),
            )
        )
    ]
    for copy in small:
        copy.start()
    for i in range(ahead):
        stream(k_ref, i, i).start()

    barrier = pltpu.get_barrier_semaphore()
    count = pages * heads
    for k in range(1, count):
        other = lax.rem(p * heads + h + k, count)
        pl.semaphore_signal(
            barrier, inc=1, device_id=(replica, other // heads, lax.rem(other, heads)), device_id_type=MESH
        )
    for copy in small:
        copy.wait()

    wide_q[...] = jnp.zeros_like(wide_q)
    for n in range(kv):
        wide_q[n * rows : (n + 1) * rows, n * depth : (n + 1) * depth] = q_ref[n]
    page_start = lax.broadcasted_iota(jnp.int32, (1, max_pages), 1) * page_rows
    slot = slot_ref[...]
    upper = jnp.where(owner_ref[...] == p, slot // per_chunk, -1)
    lower = slot % per_chunk
    upper_id = lax.broadcasted_iota(jnp.int32, (chunks, max_pages), 0)
    lower_id = lax.broadcasted_iota(jnp.int32, (per_chunk, max_pages), 0)
    table = jnp.zeros((2 * chunks, per_chunk), jnp.float32)
    for r in range(reqs):
        hit = upper[r : r + 1] == upper_id
        live = jnp.clip(len_ref[r] - page_start, 0, page_rows).astype(jnp.float32)
        left = jnp.concatenate(
            [jnp.where(hit, float(r + 1), 0.0), jnp.where(hit, live, 0.0)], axis=0
        ).astype(jnp.bfloat16)
        right = jnp.where(lower[r : r + 1] == lower_id, 1.0, 0.0).astype(jnp.bfloat16)
        table += lax.dot_general(left, right, NT, preferred_element_type=jnp.float32)
    spread = jnp.where(
        lax.broadcasted_iota(jnp.int32, (per_chunk, tokens), 1) // page_rows
        == lax.broadcasted_iota(jnp.int32, (per_chunk, tokens), 0),
        1.0,
        0.0,
    ).astype(jnp.bfloat16)
    wide = jnp.dot(table.astype(jnp.bfloat16), spread, preferred_element_type=jnp.float32)
    row_number = (lax.broadcasted_iota(jnp.int32, (chunks, tokens), 1) % page_rows).astype(jnp.float32)
    token_owner = jnp.where(row_number < wide[chunks:], wide[:chunks], 0.0)
    for c in range(chunks):
        tok[c] = jnp.broadcast_to(token_owner[c : c + 1], (8, tokens))

    req_id = (lax.broadcasted_iota(jnp.int32, (reqs, 128), 0) + 1).astype(jnp.float32)
    req_groups = reqs // 8
    mx[...] = jnp.full_like(mx, very_low)
    sub = min(tokens, 512)

    def score_chunk(c, carry):
        pl.when(c + ahead < chunks)(lambda: stream(k_ref, c + ahead, c + ahead).start())
        pl.when(c + ahead >= chunks)(lambda: stream(v_ref, c + ahead - chunks, c + ahead).start())
        at_buf = lax.rem(c, buffers)
        stream(k_ref, c, c).wait()
        groups = kv * rows // 8
        best = [mx[g * 8 // rows, g * 8 % rows : g * 8 % rows + 8] for g in range(groups)]
        for b in range(tokens // sub):
            keys = jnp.concatenate([buf[at_buf, n, b * sub : (b + 1) * sub, :] for n in range(kv)], axis=1)
            s = lax.dot_general(wide_q[...], keys, NT, preferred_element_type=jnp.float32)
            for t in range(sub // 128):
                at = b * sub + t * 128
                who = tok[c, :, at : at + 128]
                hits = [who == req_id[8 * j : 8 * j + 8] for j in range(req_groups)]
                for g in range(groups):
                    kept = jnp.where(
                        hits[g % req_groups], s[8 * g : 8 * g + 8, t * 128 : t * 128 + 128], very_low
                    )
                    s_ref[c, g * 8 // rows, g * 8 % rows : g * 8 % rows + 8, at : at + 128] = kept
                    best[g] = jnp.maximum(best[g], kept)
        for g in range(groups):
            mx[g * 8 // rows, g * 8 % rows : g * 8 % rows + 8] = best[g]
        return carry

    lax.fori_loop(0, chunks, score_chunk, 0)

    row_id = lax.broadcasted_iota(jnp.int32, (rows, 128), 0)
    lane = lax.broadcasted_iota(jnp.int32, (rows, 128), 1)
    mine_row = lax.rem(row_id, reqs) // own_reqs == p
    for n in range(kv):
        keys = jnp.concatenate([key_ref[n].astype(jnp.float32)] * group, axis=0)
        values = jnp.concatenate([value_ref[n].astype(jnp.float32)] * group, axis=0)
        self_score = jnp.sum(q_ref[n].astype(jnp.float32) * keys, axis=1, keepdims=True)
        top = jnp.max(mx[n], axis=1, keepdims=True)
        top = jnp.where(mine_row, jnp.maximum(top, self_score), top)
        take = jnp.where(mine_row, jnp.exp2((self_score - top) * factor), 0.0)
        mx[n] = top
        acc[n] = take * values
        lsum[n] = jnp.where(lane == 0, take, 0.0)

    def value_chunk(c, carry):
        i = chunks + c
        pl.when(c + ahead < chunks)(lambda: stream(v_ref, c + ahead, i + ahead).start())
        pl.when(jnp.logical_and(c + ahead >= chunks, c + ahead < chunks + pieces))(
            lambda: weight_copy(c + ahead - chunks).start()
        )
        at_buf = lax.rem(i, buffers)
        stream(v_ref, c, i).wait()
        peaks = [mx[n] for n in range(kv)]
        sums = [lsum[n] for n in range(kv)]
        outs = [acc[n] for n in range(kv)]
        for b in range(tokens // sub):
            stack = []
            for n in range(kv):
                parts = []
                for t in range(sub // 128):
                    at = b * sub + t * 128
                    w = jnp.exp2((s_ref[c, n, :, at : at + 128] - peaks[n]) * factor)
                    sums[n] += w
                    parts.append(w.astype(jnp.bfloat16))
                stack.append(jnp.concatenate(parts, axis=1))
            values = jnp.concatenate([buf[at_buf, n, b * sub : (b + 1) * sub, :] for n in range(kv)], axis=1)
            both = jnp.dot(jnp.concatenate(stack, axis=0), values, preferred_element_type=jnp.float32)
            for n in range(kv):
                outs[n] += both[n * rows : (n + 1) * rows, n * depth : (n + 1) * depth]
        for n in range(kv):
            lsum[n] = sums[n]
            acc[n] = outs[n]
        return carry

    lax.fori_loop(0, chunks, value_chunk, 0)
    for i in range(min(ahead, pieces), pieces):
        weight_copy(i).start()

    part_ref[...] = jnp.zeros_like(part_ref)
    for n in range(kv):
        stats = jnp.where(lane == 0, mx[n], jnp.sum(lsum[n], axis=1, keepdims=True))
        out = acc[n]
        for b in range(pages):
            for g in range(group):
                here = slice(g * reqs + b * own_reqs, g * reqs + (b + 1) * own_reqs)
                first = (n * group + g) * own_reqs
                part_ref[b, first : first + own_reqs, :] = out[here]
                part_ref[b, half + first : half + first + own_reqs, :] = stats[here]
    pl.semaphore_wait(barrier, count - 1)

    def exchange(k):
        to = lax.rem(p + k, pages)
        return pltpu.make_async_remote_copy(
            src_ref=part_ref.at[to],
            dst_ref=got.at[k - 1],
            send_sem=send_a.at[k - 1],
            recv_sem=recv_a.at[k - 1],
            device_id=(replica, to, h),
            device_id_type=MESH,
        )

    for k in range(1, pages):
        exchange(k).start()
    for k in range(1, pages):
        exchange(k).wait_recv()

    tops = [part_ref[p, half:, 0:1]] + [got[k, half:, 0:1] for k in range(pages - 1)]
    sums = [part_ref[p, half:, 1:2]] + [got[k, half:, 1:2] for k in range(pages - 1)]
    outs = [part_ref[p, :half]] + [got[k, :half] for k in range(pages - 1)]
    peak = tops[0]
    for t in tops[1:]:
        peak = jnp.maximum(peak, t)
    out = jnp.zeros_like(outs[0])
    weight = jnp.zeros_like(peak)
    for t, s, o in zip(tops, sums, outs):
        f = jnp.exp2((t - peak) * factor)
        out += f * o
        weight += f * s
    attended = (out / jnp.where(weight > 0.0, weight, 1.0)).astype(jnp.bfloat16)
    mine[...] = jnp.zeros_like(mine)
    mine[0:half, :] = attended

    target = p // shares
    place = lax.rem(p, shares) * heads + h

    def hand_over(k):
        to = lax.rem(p + k, pages)
        return pltpu.make_async_remote_copy(
            src_ref=mine,
            dst_ref=rows_in.at[place],
            send_sem=send_b.at[k],
            recv_sem=recv_b.at[place],
            device_id=(replica, to, target),
            device_id_type=MESH,
        )

    for k in range(pages):
        if k == 0:
            pl.when(target != h)(lambda: hand_over(0).start())

            @pl.when(target == h)
            def _():
                rows_in[place] = mine[...]
        else:
            hand_over(k).start()

    def arrival(source):
        return pltpu.make_async_remote_copy(
            src_ref=mine,
            dst_ref=rows_in.at[source],
            send_sem=send_b.at[0],
            recv_sem=recv_b.at[source],
            device_id=(replica, p, target),
            device_id_type=MESH,
        )

    for source in range(shares * heads):
        remote = jnp.logical_or(target != h, place != source)
        pl.when(remote)(lambda source=source: arrival(source).wait_recv())

    lhs[...] = jnp.zeros_like(lhs)
    per_piece = piece_rows // depth
    for source in range(shares * heads):
        first = source // heads * own_reqs
        block = rows_in[source].astype(jnp.float32)
        for n in range(head_count):
            which = source % heads * head_count + n
            col = which % per_piece * depth
            lhs[which // per_piece, first : first + own_reqs, col : col + depth] = block[
                n * own_reqs : (n + 1) * own_reqs
            ]
    total[...] = jnp.zeros_like(total)

    def multiply(i, carry):
        weight_copy(i).wait()
        total[...] += jnp.dot(
            lhs[i].astype(jnp.bfloat16), wbuf[i], preferred_element_type=jnp.float32
        )
        return carry

    lax.fori_loop(0, pieces, multiply, 0)
    y_ref[...] = total[0:out_reqs].astype(jnp.bfloat16)
    for k in range(1, pages):
        exchange(k).wait_send()
    pl.when(target != h)(lambda: hand_over(0).wait_send())
    for k in range(1, pages):
        hand_over(k).wait_send()


def local(sizes, queries, k_cache, v_cache, new_key, new_value, ctx_lens, page_owner, page_slot, out_weight):
    pages, heads = sizes
    kv, slots, page_rows, depth = k_cache.shape
    reqs, q_local, _ = queries.shape
    group = q_local // kv
    factor = math.log2(math.e) / math.sqrt(depth)
    per_chunk = math.gcd(slots, 128)
    chunks = slots // per_chunk
    tokens = per_chunk * page_rows
    rows = group * reqs
    half = round_up(kv * group * (reqs // pages), 8)
    model, columns = out_weight.shape
    pieces = math.gcd(model // depth, 8)
    sources = pages // heads * heads
    lines = round_up(half, 16)
    ahead = min(6, chunks)
    vmem = pl.BlockSpec(memory_space=pltpu.VMEM)
    hbm = pl.BlockSpec(memory_space=pl.ANY)
    return pl.pallas_call(
        functools.partial(whole_kernel, (pages, heads, page_rows, group, ahead, factor)),
        out_shape=jax.ShapeDtypeStruct((reqs // heads, columns), jnp.bfloat16),
        in_specs=[hbm] * 9,
        out_specs=vmem,
        scratch_shapes=[
            pltpu.VMEM((kv, rows, depth), jnp.bfloat16),
            pltpu.VMEM(page_owner.shape, jnp.int32),
            pltpu.VMEM(page_slot.shape, jnp.int32),
            pltpu.SMEM(ctx_lens.shape, jnp.int32),
            pltpu.VMEM(new_key.shape, jnp.bfloat16),
            pltpu.VMEM(new_value.shape, jnp.bfloat16),
            pltpu.SemaphoreType.DMA((6,)),
            pltpu.VMEM((kv * rows, kv * depth), jnp.bfloat16),
            pltpu.VMEM((ahead + 2, kv, tokens, depth), jnp.bfloat16),
            pltpu.VMEM((chunks, kv, rows, tokens), jnp.float32),
            pltpu.VMEM((chunks, 8, tokens), jnp.float32),
            pltpu.VMEM((kv, rows, 128), jnp.float32),
            pltpu.VMEM((kv, rows, depth), jnp.float32),
            pltpu.VMEM((kv, rows, 128), jnp.float32),
            pltpu.SemaphoreType.DMA((ahead + 2,)),
            pltpu.VMEM((pieces, model // pieces, columns), jnp.bfloat16),
            pltpu.VMEM((pages, 2 * half, depth), jnp.float32),
            pltpu.VMEM((pages - 1, 2 * half, depth), jnp.float32),
            pltpu.VMEM((lines, depth), jnp.bfloat16),
            pltpu.VMEM((sources, lines, depth), jnp.bfloat16),
            pltpu.VMEM((pieces, 8, model // pieces), jnp.float32),
            pltpu.VMEM((8, columns), jnp.float32),
            pltpu.SemaphoreType.DMA((pieces,)),
            pltpu.SemaphoreType.DMA((pages - 1,)),
            pltpu.SemaphoreType.DMA((pages - 1,)),
            pltpu.SemaphoreType.DMA((pages,)),
            pltpu.SemaphoreType.DMA((sources,)),
        ],
        compiler_params=pltpu.CompilerParams(
            collective_id=0, has_side_effects=True, vmem_limit_bytes=56 * 1024 * 1024
        ),
        name="decode",
    )(
        queries.transpose(1, 0, 2).reshape(kv, rows, depth),
        page_owner,
        page_slot,
        ctx_lens,
        new_key,
        new_value,
        k_cache.reshape(kv, slots * page_rows, depth),
        v_cache.reshape(kv, slots * page_rows, depth),
        out_weight,
    )


def solution(mesh):
    placed = (
        P("group", "heads", None),
        P("heads", ("group", "pages"), None, None),
        P("heads", ("group", "pages"), None, None),
        P("heads", "group", None),
        P("heads", "group", None),
        P("group"),
        P("group", None),
        P("group", None),
        P(None, "pages"),
    )
    sizes = (mesh.shape["pages"], mesh.shape["heads"])
    return jax.shard_map(
        functools.partial(local, sizes),
        mesh=mesh,
        in_specs=placed,
        out_specs=P(("group", "heads"), "pages"),
        check_vma=False,
    )
```
